32 devices in a mesh: leaf: 8 (over z, y), front: 4 (over x, core).
Axes of the slice: x: 2, y: 2, z: 4, core: 2. Of those that a mesh axis runs over, the one named last changes fastest.
Arguments:
- app_rhs: float32 [24576, 128], P(('leaf', 'front')), may hold values from -6 to 6
- pivot_source: int32 [24576], P(('leaf', 'front')), may hold values from 0 to 24575, as said below
- row_owner: int32 [24576], P(('leaf', 'front')), may hold values from 0 to 24575, as said below
- leaf_inverse: float32 [8, 4, 384, 1536], P('leaf', 'front'), may hold values from -1 to 2, as said below
- leaf_coupling: float32 [8, 4, 384, 1024], P('leaf', 'front'), may hold values from -0.07654656 to 0.07654656
- sep1_inverse: float32 [8, 4, 128, 1024], P('leaf', 'front'), may hold values from -1 to 2, as said below
- sep1_coupling: float32 [8, 4, 128, 2048], P('leaf', 'front'), may hold values from -0.09375 to 0.09375
- sep2_inverse: float32 [8, 4, 128, 2048], P('leaf', 'front'), may hold values from -1 to 2, as said below
- sep2_coupling: float32 [8, 4, 128, 4096], P('leaf', 'front'), may hold values from -0.06629126 to 0.06629126
- sep3_inverse: float32 [8, 4, 128, 4096], P('leaf', 'front'), may hold values from -1 to 2, as said below
Outputs:
- solution: float32 [24576, 128], P(('leaf', 'front'))
The draws below stay inside these ranges and needn't reach their ends.
Inputs may be any that keep to these rules, and one draw needn't show every extreme that they name: `pivot_source`: A permutation. Row e of pivot_rhs comes from a device's block of 768 application rows; one block's rows go to at most 16 blocks of pivot rows, at most 60 rows from one block to one block, and some pair of blocks carries exactly 60 rows. The inverse of pivot_source: pivot_source[row_owner[i]] = i. `leaf_inverse`: each front's matrix is the identity plus dense entries of magnitude at most 2 / sqrt of the front's pivot rows. `sep1_inverse`: as leaf_inverse. `sep2_inverse`: as leaf_inverse. `sep3_inverse`: as leaf_inverse.
All inputs are finite; a program needn't handle non-finite values.
Results may differ from the reference program's by a relative error of at most 0.00011.
Values sent between devices are 32-bit elements; how exact they have to be, the bound alone decides.
A program may use at most 128 MiB of HBM per device.

```python
import jax
import jax.numpy as jnp
from jax import lax

NRHS = 128
LEAF_PIV = 384
SEP_PIV = 128
ROWS_DEV = 768
FANOUT = 16
SPREAD = 12
NROWS = 24576
LEAF_FRONT = 1536
SEP1 = 1024
SEP2 = 2048
SEP3 = 4096
N_LEAF = 8
N_FRONT = 4


def route_tables(key):
    base_key = jax.random.fold_in(key, 7)
    keys_all = jax.random.split(base_key, 6)
    device_count = N_LEAF * N_FRONT
    row_count = ROWS_DEV
    mean_rows = ROWS_DEV // FANOUT
    labels = jax.random.permutation(keys_all[0], device_count)
    turns = jax.random.permutation(keys_all[1], device_count)
    shifts = jax.random.permutation(keys_all[2], device_count)[:FANOUT]
    offsets = jax.random.randint(keys_all[3], (FANOUT // 2,), 0, SPREAD + 1)
    offsets = offsets.at[0].set(SPREAD)
    weights = jnp.stack([mean_rows + offsets, mean_rows - offsets], axis=1).reshape(FANOUT)
    bucket_ends = jnp.cumsum(weights)
    slot_index = jnp.arange(row_count, dtype=jnp.int32)
    bucket = jnp.sum((slot_index[:, None] >= bucket_ends[None, :]).astype(jnp.int32), axis=1)
    label_of = (turns[:, None] + shifts[bucket][None, :]) % device_count
    target = jnp.argsort(labels)[label_of].astype(jnp.int32)
    local_order = jax.vmap(lambda sub_key: jax.random.permutation(sub_key, row_count))(jax.random.split(keys_all[4], device_count))
    app_row = jnp.arange(device_count, dtype=jnp.int32)[:, None] * row_count + local_order.astype(jnp.int32)
    priority = jax.random.permutation(keys_all[5], device_count * row_count).reshape(device_count, row_count).astype(jnp.int32)
    scores = (target * (device_count * row_count) + priority).reshape(-1)
    sorted_items = jnp.argsort(scores, stable=True)
    source_rows = app_row.reshape(-1)[sorted_items].astype(jnp.int32)
    owner_rows = jnp.zeros(device_count * row_count, jnp.int32).at[source_rows].set(jnp.arange(device_count * row_count, dtype=jnp.int32))
    return (source_rows, owner_rows)


def draw_pivot_source(key, part):
    return route_tables(key)[0]


def draw_row_owner(key, part):
    return route_tables(key)[1]


def draw_front(key, group_size, pivot_rows, width):
    full_shape = (N_LEAF, N_FRONT, pivot_rows, width)
    leaf_axis = jnp.arange(N_LEAF)[:, None, None, None]
    front_axis = jnp.arange(N_FRONT)[None, :, None, None]
    pivot_axis = jnp.arange(pivot_rows)[None, None, :, None]
    column_axis = jnp.arange(width)[None, None, None, :]
    diagonal_col = front_axis * (group_size * pivot_rows) + leaf_axis % group_size * pivot_rows + pivot_axis
    identity = (column_axis == diagonal_col).astype(jnp.float32)
    jitter = jnp.clip(jax.random.normal(key, full_shape, jnp.float32), -4.0, 4.0)
    return identity + 0.5 * jitter / width ** 0.5


def draw_leaf_inverse(key, part):
    return draw_front(jax.random.fold_in(key, 11), 1, LEAF_PIV, LEAF_FRONT)


def draw_sep1_inverse(key, part):
    return draw_front(jax.random.fold_in(key, 12), 2, SEP_PIV, SEP1)


def draw_sep2_inverse(key, part):
    return draw_front(jax.random.fold_in(key, 13), 4, SEP_PIV, SEP2)


def draw_sep3_inverse(key, part):
    return draw_front(jax.random.fold_in(key, 14), 8, SEP_PIV, SEP3)


def block_scale(stream_key, extent, cuts, least, high):
    gain, own = 1.0, jax.random.fold_in(stream_key, 6)
    for axis_at, shards_of in cuts:
        draws = jnp.exp(jax.random.uniform(jax.random.fold_in(own, axis_at), (shards_of,), jnp.float32, least / len(cuts), high / len(cuts)))
        gain = gain * jnp.repeat(draws, extent[axis_at] // shards_of).reshape([-1 if axis == axis_at else 1 for axis in range(len(extent))])
    return gain


def noise(own_key, extent, spread, limit, shards=(), kind=jnp.bfloat16):
    gain = block_scale(own_key, extent, shards, -0.22, 0.18) if shards else 1.0
    drawn = jax.random.normal(own_key, extent, jnp.float32) * spread * gain
    return jnp.minimum(jnp.maximum(drawn, -limit), limit).astype(kind)


def setup_inputs(seed: int = 0) -> dict:
    streams_of = jax.random.split(jax.random.key(seed), 11)
    return {
        "app_rhs": noise(streams_of[0], (NROWS, NRHS), 1.0, 6.0, ((0, 32),), jnp.float32),
        "pivot_source": draw_pivot_source(jax.random.fold_in(streams_of[10], 71), 0),
        "row_owner": draw_row_owner(jax.random.fold_in(streams_of[10], 71), 0),
        "leaf_inverse": draw_leaf_inverse(jax.random.fold_in(streams_of[10], 71), 0),
        "leaf_coupling": noise(streams_of[4], (N_LEAF, N_FRONT, LEAF_PIV, SEP1), (0.5 * LEAF_FRONT ** -0.5), 0.07654656, ((0, 8), (1, 4)), jnp.float32),
        "sep1_inverse": draw_sep1_inverse(jax.random.fold_in(streams_of[10], 71), 0),
        "sep1_coupling": noise(streams_of[6], (N_LEAF, N_FRONT, SEP_PIV, SEP2), (0.5 * SEP1 ** -0.5), 0.09375, ((0, 8), (1, 4)), jnp.float32),
        "sep2_inverse": draw_sep2_inverse(jax.random.fold_in(streams_of[10], 71), 0),
        "sep2_coupling": noise(streams_of[8], (N_LEAF, N_FRONT, SEP_PIV, SEP3), (0.5 * SEP2 ** -0.5), 0.06629126, ((0, 8), (1, 4)), jnp.float32),
        "sep3_inverse": draw_sep3_inverse(jax.random.fold_in(streams_of[10], 71), 0),
    }


PRECISE = lax.Precision.HIGHEST


def node_form(blocked, group_size):
    leaves, fronts, pivot_rows, col_count = blocked.shape
    shaped = blocked.reshape(leaves // group_size, group_size, fronts, pivot_rows, col_count)
    shaped = jnp.transpose(shaped, (0, 2, 1, 3, 4))
    return shaped.reshape(leaves // group_size, fronts * group_size * pivot_rows, col_count)


def device_form(nodes, group_size, fronts, pivot_rows):
    node_count, row_count, col_count = nodes.shape
    shaped = nodes.reshape(node_count, fronts, group_size, pivot_rows, col_count)
    shaped = jnp.transpose(shaped, (0, 2, 1, 3, 4))
    return shaped.reshape(node_count * group_size, fronts, pivot_rows, col_count)


def apply_rows(matrices, vectors):
    return jnp.einsum("nab,nbc->nac", matrices, vectors, precision=PRECISE)


def apply_cols(matrices, vectors):
    return jnp.einsum("nba,nbc->nac", matrices, vectors, precision=PRECISE)


def pair_sum(partials):
    node_count, row_count, col_count = partials.shape
    return partials.reshape(node_count // 2, 2, row_count, col_count).sum(axis=1)


def reference(app_rhs, pivot_source, row_owner, leaf_inverse, leaf_coupling, sep1_inverse, sep1_coupling, sep2_inverse, sep2_coupling, sep3_inverse):
    leaves = leaf_inverse.shape[0]
    fronts = leaf_inverse.shape[1]
    ordered = app_rhs[pivot_source].reshape(leaves, fronts, ROWS_DEV, NRHS)
    inverses = [leaf_inverse, sep1_inverse, sep2_inverse, sep3_inverse]
    couplings = [leaf_coupling, sep1_coupling, sep2_coupling]
    pivots = [LEAF_PIV, SEP_PIV, SEP_PIV, SEP_PIV]
    starts = [0, LEAF_PIV, LEAF_PIV + SEP_PIV, LEAF_PIV + 2 * SEP_PIV]
    solved = []
    carried = None
    for height in range(4):
        group_size = 2 ** height
        own_rhs = node_form(ordered[:, :, starts[height]:starts[height] + pivots[height]], group_size)
        if height > 0:
            own_rhs = own_rhs - carried
        forward = apply_rows(node_form(inverses[height], group_size), own_rhs)
        solved.append(forward)
        if height < 3:
            carried = pair_sum(apply_cols(node_form(couplings[height], group_size), forward))
    pieces = [None, None, None, None]
    parent_sol = None
    for height in (3, 2, 1, 0):
        group_size = 2 ** height
        target = solved[height]
        if height < 3:
            target = target - apply_rows(node_form(couplings[height], group_size), jnp.repeat(parent_sol, 2, axis=0))
        parent_sol = apply_cols(node_form(inverses[height], group_size), target)
        pieces[height] = device_form(parent_sol, group_size, fronts, pivots[height])
    pivot_order = jnp.concatenate(pieces, axis=2).reshape(leaves * fronts * ROWS_DEV, NRHS)
    return pivot_order[row_owner]
```

```python
import functools

import jax
import jax.numpy as jnp
from jax import lax
from jax.experimental import pallas as pl
from jax.experimental.pallas import tpu as pltpu
from jax.sharding import PartitionSpec as P

LEAF_PIV = 384
SEP_PIV = 128
BLK = 128
CHUNK = 4
MESH = pl.DeviceIdType.MESH


def ranked_slots(targets, bucket_count):
    one_hot = (targets[:, None] == jnp.arange(bucket_count, dtype=jnp.int32)[None, :]).astype(
        jnp.int32
    )
    running = jnp.cumsum(one_hot, axis=0) - one_hot
    return jnp.sum(running * one_hot, axis=1)


def move_rows(outgoing, slot_cap):
    leaves = lax.axis_size("leaf")
    fronts = lax.axis_size("front")
    rhs_count = outgoing.shape[1]
    shaped = outgoing.reshape(leaves * fronts, slot_cap, rhs_count)
    arrived = lax.all_to_all(shaped, ("leaf", "front"), split_axis=0, concat_axis=0, tiled=True)
    return arrived.reshape(leaves * fronts * slot_cap, rhs_count)


def bit_of(value, place):
    return lax.rem(lax.div(value, jnp.int32(2**place)), jnp.int32(2))


def stripe_orders(front_bits, height):
    front = [("front", place) for place in range(front_bits)]
    leaf = [("leaf", place) for place in range(height)]
    first = front + leaf
    second = front[:1] + leaf[:1] + front[1:] + leaf[1:]
    return (first, second)


def split(value):
    high = value.astype(jnp.bfloat16)
    return high, (value - high.astype(jnp.float32)).astype(jnp.bfloat16)


def product(left, right, right_axis):
    dims = (((1,), (right_axis,)), ((), ()))
    dot = functools.partial(lax.dot_general, dimension_numbers=dims, preferred_element_type=jnp.float32)
    left_high, left_low = left
    right_high, right_low = split(right)
    return dot(left_high, right_high) + (dot(left_low, right_high) + dot(left_high, right_low))


def solve_kernel(front_bits, stripe_rows, sizes, *refs):
    rhs_ref, *weights_hbm = refs[:8]
    out_ref = refs[8]
    weights = refs[9:16]
    buffers = refs[16:]
    stripes = len(stripe_rows)
    pos = 0

    def take(count):
        nonlocal pos
        pos += count
        return buffers[pos - count : pos]

    up = [take(stripes) for _ in range(4)]
    down = [None] + [take(stripes) for _ in range(3)]
    partial = take(stripes)
    up_recv = [None] + [take(stripes) for _ in range(3)]
    down_recv = [take(stripes) for _ in range(4)]
    solved = take(4)
    load_sems, send_sems, recv_sems = take(3)
    used = [0]

    leaf = lax.axis_index("leaf")
    front = lax.axis_index("front")
    here = {"leaf": leaf, "front": front}

    def partner(bit):
        axis, place = bit
        mine = bit_of(here[axis], place)
        other = here[axis] + (1 - 2 * mine) * 2**place
        return (other, front) if axis == "leaf" else (leaf, other)

    all_bits = [("front", place) for place in range(front_bits)] + [("leaf", place) for place in range(3)]
    barrier = pltpu.get_barrier_semaphore()
    for bit in all_bits:
        pl.semaphore_signal(barrier, inc=1, device_id=partner(bit), device_id_type=MESH)
    loads = []
    for index in range(7):
        load = pltpu.make_async_copy(weights_hbm[index], weights[index], load_sems.at[index])
        load.start()
        loads.append(load)
    pl.semaphore_wait(barrier, len(all_bits))

    def unit(height):
        return LEAF_PIV // BLK if height == 0 else 1

    def slot_of(block, height, stripe):
        piece = unit(height)
        place, rest = (block, 0) if piece == 1 else (lax.div(block, jnp.int32(piece)), lax.rem(block, jnp.int32(piece)))
        order = stripe_orders(front_bits, height)[stripe]
        slot = 0
        for axis, at in order:
            slot = slot * 2 + bit_of(place, at + height if axis == "front" else at)
        return slot * piece + rest

    def remote(source, target, bit):
        index = used[0]
        used[0] += 1
        copy = pltpu.make_async_remote_copy(
            src_ref=source,
            dst_ref=target,
            send_sem=send_sems.at[index],
            recv_sem=recv_sems.at[index],
            device_id=partner(bit),
            device_id_type=MESH,
        )
        copy.start()
        return copy

    def own_slots(height):
        out = []
        for stripe in range(stripes):
            slot = 0
            for axis, at in stripe_orders(front_bits, height)[stripe]:
                slot = slot * 2 + bit_of(here[axis], at)
            out.append(slot * unit(height))
        return out

    def reduce_group(height, bufs, recvs):
        piece = unit(height)
        orders = stripe_orders(front_bits, height)
        depth = len(orders[0])
        bases = [jnp.int32(0)] * stripes
        half = 2**depth * piece
        offset = 0
        for step in range(depth + 1):
            copies = []
            whole, half = half, half // 2
            for stripe in range(stripes):
                if step > 0:
                    pending[stripe].wait()
                    keep = bases[stripe]

                    def add(index, carry, stripe=stripe, keep=keep, prior=prior):
                        bufs[stripe][keep + index] += recvs[stripe][prior + index]
                        return carry

                    lax.fori_loop(0, whole, add, 0)
                if step < depth:
                    bit = orders[stripe][step]
                    mine = bit_of(here[bit[0]], bit[1])
                    away = bases[stripe] + (1 - mine) * half
                    bases[stripe] = bases[stripe] + mine * half
                    copies.append(
                        remote(bufs[stripe].at[pl.ds(away, half)], recvs[stripe].at[pl.ds(offset, half)], bit)
                    )
            pending, prior = copies, offset
            offset += half

    def gather_group(height, bufs):
        piece = unit(height)
        orders = stripe_orders(front_bits, height)
        depth = len(orders[0])
        bases = own_slots(height)
        size = piece
        pending = None
        for step in range(depth, -1, -1):
            copies = []
            for stripe in range(stripes):
                if pending is not None:
                    pending[stripe].wait()
                if step > 0:
                    bit = orders[stripe][step - 1]
                    span = pl.ds(bases[stripe], size)
                    copies.append(remote(bufs[stripe].at[span], bufs[stripe].at[span], bit))
                    bases[stripe] = bases[stripe] - bit_of(here[bit[0]], bit[1]) * size
            pending = copies
            size *= 2

    def apply_rows(weight, bufs, height):
        rows = weight.shape[0]
        count = sizes[height] // BLK

        def body(index, total):
            parts = []
            for step in range(CHUNK):
                block = index * CHUNK + step
                parts.append(
                    jnp.concatenate([bufs[s][slot_of(block, height, s)] for s in range(stripes)], axis=0)
                )
            left = split(jnp.concatenate(parts, axis=1))
            start = pl.multiple_of(index * (CHUNK * BLK), CHUNK * BLK)
            return total + product(left, weight[:, pl.ds(start, CHUNK * BLK)], 1)

        return lax.fori_loop(0, count // CHUNK, body, jnp.zeros((BLK, rows), jnp.float32))

    def apply_cols(weight, vector, bufs, height):
        count = sizes[height] // BLK
        left = split(vector)

        def body(index, carry):
            start = pl.multiple_of(index * (CHUNK * BLK), CHUNK * BLK)
            result = product(left, weight[:, pl.ds(start, CHUNK * BLK)], 0)
            for step in range(CHUNK):
                block = index * CHUNK + step
                low = 0
                for s in range(stripes):
                    bufs[s][slot_of(block, height, s)] = result[
                        low : low + stripe_rows[s], step * BLK : (step + 1) * BLK
                    ]
                    low += stripe_rows[s]
            return carry

        lax.fori_loop(0, count // CHUNK, body, 0)

    def own_block(bufs, slots, part):
        return jnp.concatenate([bufs[s][slots[s] + part] for s in range(stripes)], axis=0)

    def set_block(bufs, slots, part, value):
        low = 0
        for s in range(stripes):
            bufs[s][slots[s] + part] = value[low : low + stripe_rows[s]]
            low += stripe_rows[s]

    inverses = (weights[0], weights[2], weights[4], weights[6])
    couplings = (weights[1], weights[3], weights[5])
    starts = (0, LEAF_PIV, LEAF_PIV + SEP_PIV, LEAF_PIV + 2 * SEP_PIV)
    for height in range(4):
        slots = own_slots(height)
        if height > 0:
            reduce_group(height, partial, up_recv[height])
        for part in range(unit(height)):
            low = starts[height] + part * BLK
            value = rhs_ref[low : low + BLK, :].T
            if height > 0:
                value = value - own_block(partial, slots, part)
            set_block(up[height], slots, part, value)
        gather_group(height, up[height])
        loads[2 * height].wait()
        forward = apply_rows(inverses[height], up[height], height)
        solved[height][...] = forward
        if height < 3:
            loads[2 * height + 1].wait()
            apply_cols(couplings[height], forward, partial, height + 1)
    for height in (3, 2, 1, 0):
        target = solved[height][...]
        if height < 3:
            target = target - apply_rows(couplings[height], down[height + 1], height + 1)
        apply_cols(inverses[height], target, partial, height)
        reduce_group(height, partial, down_recv[height])
        slots = own_slots(height)
        for part in range(unit(height)):
            low = starts[height] + part * BLK
            value = own_block(partial, slots, part)
            out_ref[low : low + BLK, :] = value.T
            if height > 0:
                set_block(down[height], slots, part, value)
        if height > 0:
            gather_group(height, down[height])


def solve(ordered, weights):
    leaves = lax.axis_size("leaf")
    fronts = lax.axis_size("front")
    front_bits = fronts.bit_length() - 1
    rhs_count = ordered.shape[1]
    stripe_rows = (rhs_count // 2, rhs_count // 2)
    sizes = tuple(w.shape[1] for w in (weights[0], weights[2], weights[4], weights[6]))
    scratch = [pltpu.VMEM(w.shape, jnp.float32) for w in weights]

    def stripe_buffers(blocks):
        return [pltpu.VMEM((blocks, rows, BLK), jnp.float32) for rows in stripe_rows]

    counts = [size // BLK for size in sizes]
    copies = 0
    for height in range(4):
        copies += (2 if height == 0 else 4) * (front_bits + height) * len(stripe_rows)
    for blocks in counts + counts[1:] + [max(counts)] + counts[1:] + counts:
        scratch += stripe_buffers(blocks)
    scratch += [pltpu.VMEM((rhs_count, rows), jnp.float32) for rows in (LEAF_PIV, SEP_PIV, SEP_PIV, SEP_PIV)]
    scratch += [
        pltpu.SemaphoreType.DMA((7,)),
        pltpu.SemaphoreType.DMA((copies,)),
        pltpu.SemaphoreType.DMA((copies,)),
    ]
    vmem = pl.BlockSpec(memory_space=pltpu.VMEM)
    return pl.pallas_call(
        functools.partial(solve_kernel, front_bits, stripe_rows, sizes),
        out_shape=jax.ShapeDtypeStruct(ordered.shape, jnp.float32),
        in_specs=[vmem] + [pl.BlockSpec(memory_space=pl.ANY)] * 7,
        out_specs=vmem,
        scratch_shapes=scratch,
        compiler_params=pltpu.CompilerParams(
            collective_id=0, has_side_effects=True, vmem_limit_bytes=66 * 1024 * 1000
        ),
    )(ordered, *weights)


def per_device(
    app_rhs,
    pivot_source,
    row_owner,
    leaf_inverse,
    leaf_coupling,
    sep1_inverse,
    sep1_coupling,
    sep2_inverse,
    sep2_coupling,
    sep3_inverse,
):
    row_count = app_rhs.shape[0]
    rhs_count = app_rhs.shape[1]
    peer_count = lax.axis_size("leaf") * lax.axis_size("front")
    mean_rows = row_count // (peer_count // 2)
    slot_cap = mean_rows + max(1, mean_rows // 4)
    destination = row_owner // row_count
    send_index = destination * slot_cap + ranked_slots(destination, peer_count)
    anchor = pivot_source // row_count
    same_source = (anchor[:, None] == anchor[None, :]) & (
        pivot_source[None, :] < pivot_source[:, None]
    )
    recv_index = anchor * slot_cap + jnp.sum(same_source.astype(jnp.int32), axis=1)
    outgoing = (
        jnp.zeros((peer_count * slot_cap, rhs_count), jnp.float32).at[send_index].set(app_rhs)
    )
    ordered = move_rows(outgoing, slot_cap)[recv_index]
    weights = [
        w[0, 0]
        for w in (
            leaf_inverse,
            leaf_coupling,
            sep1_inverse,
            sep1_coupling,
            sep2_inverse,
            sep2_coupling,
            sep3_inverse,
        )
    ]
    pivot_order = solve(ordered, weights)
    returning = (
        jnp.zeros((peer_count * slot_cap, rhs_count), jnp.float32).at[recv_index].set(pivot_order)
    )
    returned = move_rows(returning, slot_cap)
    return returned[send_index]


def solution(mesh):
    in_specs = (
        P(("leaf", "front"), None),
        P(("leaf", "front")),
        P(("leaf", "front")),
        P("leaf", "front", None, None),
        P("leaf", "front", None, None),
        P("leaf", "front", None, None),
        P("leaf", "front", None, None),
        P("leaf", "front", None, None),
        P("leaf", "front", None, None),
        P("leaf", "front", None, None),
    )
    out_specs = P(("leaf", "front"), None)
    return jax.shard_map(
        per_device, mesh=mesh, in_specs=in_specs, out_specs=out_specs, check_vma=False
    )
```

```python
import functools

import jax
import jax.numpy as jnp
from jax import lax
from jax.experimental import pallas as pl
from jax.experimental.pallas import tpu as pltpu
from jax.sharding import PartitionSpec as P

LEAF_PIV = 384
SEP_PIV = 128
BLK = 128
CHUNK = 4
STRIPES = 4
MESH = pl.DeviceIdType.MESH


def ranked_slots(targets, bucket_count):
    one_hot = (targets[:, None] == jnp.arange(bucket_count, dtype=jnp.int32)[None, :]).astype(
        jnp.int32
    )
    running = jnp.cumsum(one_hot, axis=0) - one_hot
    return jnp.sum(running * one_hot, axis=1)


def move_rows(outgoing, slot_cap):
    leaves = lax.axis_size("leaf")
    fronts = lax.axis_size("front")
    rhs_count = outgoing.shape[1]
    shaped = outgoing.reshape(leaves * fronts, slot_cap, rhs_count)
    arrived = lax.all_to_all(shaped, ("leaf", "front"), split_axis=0, concat_axis=0, tiled=True)
    return arrived.reshape(leaves * fronts * slot_cap, rhs_count)


def bit_of(value, place):
    return lax.rem(lax.div(value, jnp.int32(2**place)), jnp.int32(2))


def stripe_orders(front_bits, height):
    front = [("front", place) for place in range(front_bits)]
    leaf = [("leaf", place) for place in range(height)]
    first = front + leaf
    second = front[:1] + leaf[:1] + front[1:] + leaf[1:]
    return (first, second)


def split(value):
    high = value.astype(jnp.bfloat16)
    return high, (value - high.astype(jnp.float32)).astype(jnp.bfloat16)


def product(left, right, right_axis):
    dims = (((1,), (right_axis,)), ((), ()))
    dot = functools.partial(lax.dot_general, dimension_numbers=dims, preferred_element_type=jnp.float32)
    left_high, left_low = left
    right_high, right_low = split(right)
    return dot(left_high, right_high) + (dot(left_low, right_high) + dot(left_high, right_low))


def solve_kernel(front_bits, stripe_rows, sizes, *refs):
    rhs_ref, *weights_hbm = refs[:8]
    out_ref = refs[8]
    weights = refs[9:16]
    buffers = refs[16:]
    stripes = len(stripe_rows)
    pos = 0

    def take(count):
        nonlocal pos
        pos += count
        return buffers[pos - count : pos]

    up = [take(stripes) for _ in range(4)]
    down = [None] + [take(stripes) for _ in range(3)]
    partial = take(stripes)
    up_recv = [None] + [take(stripes) for _ in range(3)]
    down_recv = [take(stripes) for _ in range(4)]
    solved = take(4)
    load_sems, send_sems, recv_sems = take(3)
    used = [0]

    leaf = lax.axis_index("leaf")
    front = lax.axis_index("front")
    here = {"leaf": leaf, "front": front}

    def partner(bit):
        axis, place = bit
        mine = bit_of(here[axis], place)
        other = here[axis] + (1 - 2 * mine) * 2**place
        return (other, front) if axis == "leaf" else (leaf, other)

    all_bits = [("front", place) for place in range(front_bits)] + [("leaf", place) for place in range(3)]
    barrier = pltpu.get_barrier_semaphore()
    for bit in all_bits:
        pl.semaphore_signal(barrier, inc=1, device_id=partner(bit), device_id_type=MESH)
    loads = []
    for index in range(7):
        load = pltpu.make_async_copy(weights_hbm[index], weights[index], load_sems.at[index])
        load.start()
        loads.append(load)
    pl.semaphore_wait(barrier, len(all_bits))

    def unit(height):
        return LEAF_PIV // BLK if height == 0 else 1

    def slot_of(block, height, stripe):
        piece = unit(height)
        static = isinstance(block, int)
        place, rest = divmod(block, piece) if static else (block, 0)
        order = stripe_orders(front_bits, height)[stripe % 2]
        slot = 0
        for axis, at in order:
            at = at + height if axis == "front" else at
            slot = slot * 2 + (place >> at & 1 if static else bit_of(place, at))
        return slot * piece + rest

    def remote(source, target, bit):
        index = used[0]
        used[0] += 1
        copy = pltpu.make_async_remote_copy(
            src_ref=source,
            dst_ref=target,
            send_sem=send_sems.at[index],
            recv_sem=recv_sems.at[index],
            device_id=partner(bit),
            device_id_type=MESH,
        )
        copy.start()
        return copy

    def own_slots(height):
        out = []
        for stripe in range(stripes):
            slot = 0
            for axis, at in stripe_orders(front_bits, height)[stripe % 2]:
                slot = slot * 2 + bit_of(here[axis], at)
            out.append(slot * unit(height))
        return out

    def reduce_group(height, bufs, recvs, middle):
        piece = unit(height)
        orders = stripe_orders(front_bits, height)
        depth = len(orders[0])
        bases = [jnp.int32(0)] * stripes
        half = 2**depth * piece
        offset = 0
        for step in range(depth + 1):
            copies = []
            whole, half = half, half // 2
            for stripe in range(stripes):
                if step > 0:
                    pending[stripe].wait()
                    keep = bases[stripe]

                    def add(index, carry, stripe=stripe, keep=keep, prior=prior):
                        bufs[stripe][keep + index] += recvs[stripe][prior + index]
                        return carry

                    lax.fori_loop(0, whole, add, 0)
                if step < depth:
                    bit = orders[stripe % 2][step]
                    mine = bit_of(here[bit[0]], bit[1])
                    away = bases[stripe] + (1 - mine) * half
                    bases[stripe] = bases[stripe] + mine * half
                    copies.append(
                        remote(bufs[stripe].at[pl.ds(away, half)], recvs[stripe].at[pl.ds(offset, half)], bit)
                    )
            if step == 0:
                middle()
            pending, prior = copies, offset
            offset += half

    def gather_group(height, bufs, middle):
        piece = unit(height)
        orders = stripe_orders(front_bits, height)
        depth = len(orders[0])
        bases = own_slots(height)
        size = piece
        pending = None
        for step in range(depth, -1, -1):
            copies = []
            if step == 0:
                middle()
            for stripe in range(stripes):
                if pending is not None:
                    pending[stripe].wait()
                if step > 0:
                    bit = orders[stripe % 2][step - 1]
                    span = pl.ds(bases[stripe], size)
                    copies.append(remote(bufs[stripe].at[span], bufs[stripe].at[span], bit))
                    bases[stripe] = bases[stripe] - bit_of(here[bit[0]], bit[1]) * size
            pending = copies
            size *= 2

    def splits(height):
        return unit(height) == 1 and 2**height % CHUNK == 0

    def chunks(height, side, body, carry):
        count = sizes[height] // BLK // CHUNK
        if unit(height) > 1:
            for index in range(count):
                slots = [
                    [slot_of(index * CHUNK + step, height, kind) for kind in range(2)] for step in range(CHUNK)
                ]
                carry = body(index * CHUNK * BLK, slots, carry)
            return carry

        def visit(index, carry):
            if side is not None:
                run = 2**height // CHUNK
                index = lax.div(index, jnp.int32(run)) * (2 * run) + side * run + lax.rem(index, jnp.int32(run))
            bases = [slot_of(index * CHUNK, height, kind) for kind in range(2)]
            slots = [[bases[kind] + slot_of(step, height, kind) for kind in range(2)] for step in range(CHUNK)]
            return body(pl.multiple_of(index * (CHUNK * BLK), CHUNK * BLK), slots, carry)

        return lax.fori_loop(0, count if side is None else count // 2, visit, carry)

    def apply_rows(weight, bufs, height, side, total):
        def body(start, slots, total):
            parts = [
                jnp.concatenate([bufs[s][slots[step][s % 2]] for s in range(stripes)], axis=0)
                for step in range(CHUNK)
            ]
            left = split(jnp.concatenate(parts, axis=1))
            return total + product(left, weight[:, pl.ds(start, CHUNK * BLK)], 1)

        return chunks(height, side, body, total)

    def apply_cols(weight, vector, bufs, height, side):
        left = split(vector)

        def body(start, slots, carry):
            result = product(left, weight[:, pl.ds(start, CHUNK * BLK)], 0)
            for step in range(CHUNK):
                low = 0
                for s in range(stripes):
                    bufs[s][slots[step][s % 2]] = result[low : low + stripe_rows[s], step * BLK : (step + 1) * BLK]
                    low += stripe_rows[s]
            return carry

        chunks(height, side, body, 0)

    core = bit_of(front, 0)

    def reduced(weight, vector, height, recvs):
        if splits(height):
            apply_cols(weight, vector, partial, height, 1 - core)
            reduce_group(
                height, partial, recvs, lambda: apply_cols(weight, vector, partial, height, core)
            )
        else:
            apply_cols(weight, vector, partial, height, None)
            reduce_group(height, partial, recvs, lambda: None)

    def gathered_rows(weight, bufs, height, ready):
        totals = [jnp.zeros((BLK, weight.shape[0]), jnp.float32)]

        def own_side():
            ready()
            if splits(height):
                totals.append(apply_rows(weight, bufs, height, core, totals[-1]))

        gather_group(height, bufs, own_side)
        return apply_rows(weight, bufs, height, 1 - core if splits(height) else None, totals[-1])

    def own_block(bufs, slots, part):
        return jnp.concatenate([bufs[s][slots[s] + part] for s in range(stripes)], axis=0)

    def set_block(bufs, slots, part, value):
        low = 0
        for s in range(stripes):
            bufs[s][slots[s] + part] = value[low : low + stripe_rows[s]]
            low += stripe_rows[s]

    inverses = (weights[0], weights[2], weights[4], weights[6])
    couplings = (weights[1], weights[3], weights[5])
    starts = (0, LEAF_PIV, LEAF_PIV + SEP_PIV, LEAF_PIV + 2 * SEP_PIV)
    for height in range(4):
        slots = own_slots(height)
        if height > 0:
            loads[2 * height - 1].wait()
            reduced(couplings[height - 1], solved[height - 1][...], height, up_recv[height])
        for part in range(unit(height)):
            low = starts[height] + part * BLK
            value = rhs_ref[low : low + BLK, :].T
            if height > 0:
                value = value - own_block(partial, slots, part)
            set_block(up[height], slots, part, value)
        solved[height][...] = gathered_rows(inverses[height], up[height], height, loads[2 * height].wait)
    for height in (3, 2, 1, 0):
        target = solved[height][...]
        if height < 3:
            target = target - gathered_rows(couplings[height], down[height + 1], height + 1, lambda: None)
        reduced(inverses[height], target, height, down_recv[height])
        slots = own_slots(height)
        for part in range(unit(height)):
            low = starts[height] + part * BLK
            value = own_block(partial, slots, part)
            out_ref[low : low + BLK, :] = value.T
            if height > 0:
                set_block(down[height], slots, part, value)


def solve(ordered, weights):
    leaves = lax.axis_size("leaf")
    fronts = lax.axis_size("front")
    front_bits = fronts.bit_length() - 1
    rhs_count = ordered.shape[1]
    stripe_rows = (rhs_count // STRIPES,) * STRIPES
    sizes = tuple(w.shape[1] for w in (weights[0], weights[2], weights[4], weights[6]))
    scratch = [pltpu.VMEM(w.shape, jnp.float32) for w in weights]

    def stripe_buffers(blocks):
        return [pltpu.VMEM((blocks, rows, BLK), jnp.float32) for rows in stripe_rows]

    counts = [size // BLK for size in sizes]
    copies = 0
    for height in range(4):
        copies += (2 if height == 0 else 4) * (front_bits + height) * len(stripe_rows)
    for blocks in counts + counts[1:] + [max(counts)] + counts[1:] + counts:
        scratch += stripe_buffers(blocks)
    scratch += [pltpu.VMEM((rhs_count, rows), jnp.float32) for rows in (LEAF_PIV, SEP_PIV, SEP_PIV, SEP_PIV)]
    scratch += [
        pltpu.SemaphoreType.DMA((7,)),
        pltpu.SemaphoreType.DMA((copies,)),
        pltpu.SemaphoreType.DMA((copies,)),
    ]
    vmem = pl.BlockSpec(memory_space=pltpu.VMEM)
    return pl.pallas_call(
        functools.partial(solve_kernel, front_bits, stripe_rows, sizes),
        out_shape=jax.ShapeDtypeStruct(ordered.shape, jnp.float32),
        in_specs=[vmem] + [pl.BlockSpec(memory_space=pl.ANY)] * 7,
        out_specs=vmem,
        scratch_shapes=scratch,
        compiler_params=pltpu.CompilerParams(
            collective_id=0, has_side_effects=True, vmem_limit_bytes=66 * 1024 * 1000
        ),
    )(ordered, *weights)


def per_device(
    app_rhs,
    pivot_source,
    row_owner,
    leaf_inverse,
    leaf_coupling,
    sep1_inverse,
    sep1_coupling,
    sep2_inverse,
    sep2_coupling,
    sep3_inverse,
):
    row_count = app_rhs.shape[0]
    rhs_count = app_rhs.shape[1]
    peer_count = lax.axis_size("leaf") * lax.axis_size("front")
    mean_rows = row_count // (peer_count // 2)
    slot_cap = mean_rows + max(1, mean_rows // 4)
    destination = row_owner // row_count
    send_index = destination * slot_cap + ranked_slots(destination, peer_count)
    anchor = pivot_source // row_count
    same_source = (anchor[:, None] == anchor[None, :]) & (
        pivot_source[None, :] < pivot_source[:, None]
    )
    recv_index = anchor * slot_cap + jnp.sum(same_source.astype(jnp.int32), axis=1)
    outgoing = (
        jnp.zeros((peer_count * slot_cap, rhs_count), jnp.float32).at[send_index].set(app_rhs)
    )
    ordered = move_rows(outgoing, slot_cap)[recv_index]
    weights = [
        w[0, 0]
        for w in (
            leaf_inverse,
            leaf_coupling,
            sep1_inverse,
            sep1_coupling,
            sep2_inverse,
            sep2_coupling,
            sep3_inverse,
        )
    ]
    pivot_order = solve(ordered, weights)
    returning = (
        jnp.zeros((peer_count * slot_cap, rhs_count), jnp.float32).at[recv_index].set(pivot_order)
    )
    returned = move_rows(returning, slot_cap)
    return returned[send_index]


def solution(mesh):
    in_specs = (
        P(("leaf", "front"), None),
        P(("leaf", "front")),
        P(("leaf", "front")),
        P("leaf", "front", None, None),
        P("leaf", "front", None, None),
        P("leaf", "front", None, None),
        P("leaf", "front", None, None),
        P("leaf", "front", None, None),
        P("leaf", "front", None, None),
        P("leaf", "front", None, None),
    )
    out_specs = P(("leaf", "front"), None)
    return jax.shard_map(
        per_device, mesh=mesh, in_specs=in_specs, out_specs=out_specs, check_vma=False
    )
```

```python
import functools

import jax
import jax.numpy as jnp
from jax import lax
from jax.experimental import pallas as pl
from jax.experimental.pallas import tpu as pltpu
from jax.sharding import PartitionSpec as P

LEAF_PIV = 384
SEP_PIV = 128
BLK = 128
CHUNK = 4
STRIPES = 8
MESH = pl.DeviceIdType.MESH


def ranked_slots(targets, bucket_count):
    one_hot = (targets[:, None] == jnp.arange(bucket_count, dtype=jnp.int32)[None, :]).astype(
        jnp.int32
    )
    running = jnp.cumsum(one_hot, axis=0) - one_hot
    return jnp.sum(running * one_hot, axis=1)


def move_rows(outgoing, slot_cap):
    leaves = lax.axis_size("leaf")
    fronts = lax.axis_size("front")
    rhs_count = outgoing.shape[1]
    shaped = outgoing.reshape(leaves * fronts, slot_cap, rhs_count)
    arrived = lax.all_to_all(shaped, ("leaf", "front"), split_axis=0, concat_axis=0, tiled=True)
    return arrived.reshape(leaves * fronts * slot_cap, rhs_count)


def bit_of(value, place):
    return lax.rem(lax.div(value, jnp.int32(2**place)), jnp.int32(2))


def stripe_orders(front_bits, height):
    front = [("front", place) for place in range(front_bits)]
    leaf = [("leaf", place) for place in range(height)]
    first = front + leaf
    second = front[:1] + leaf[:1] + front[1:] + leaf[1:]
    return (first, second)


def split(value):
    high = value.astype(jnp.bfloat16)
    return high, (value - high.astype(jnp.float32)).astype(jnp.bfloat16)


def product(left, right, right_axis):
    dims = (((1,), (right_axis,)), ((), ()))
    dot = functools.partial(lax.dot_general, dimension_numbers=dims, preferred_element_type=jnp.float32)
    left_high, left_low = left
    right_high, right_low = split(right)
    return dot(left_high, right_high) + (dot(left_low, right_high) + dot(left_high, right_low))


def solve_kernel(front_bits, stripe_rows, sizes, *refs):
    rhs_ref, *weights_hbm = refs[:8]
    out_ref = refs[8]
    weights = refs[9:16]
    buffers = refs[16:]
    stripes = len(stripe_rows)
    pos = 0

    def take(count):
        nonlocal pos
        pos += count
        return buffers[pos - count : pos]

    up = [take(stripes) for _ in range(4)]
    down = [None] + [take(stripes) for _ in range(3)]
    partial = take(stripes)
    up_recv = [None] + [take(stripes) for _ in range(3)]
    down_recv = [take(stripes) for _ in range(4)]
    solved = take(4)
    load_sems, send_sems, recv_sems = take(3)
    used = [0]

    leaf = lax.axis_index("leaf")
    front = lax.axis_index("front")
    here = {"leaf": leaf, "front": front}

    def partner(bit):
        axis, place = bit
        mine = bit_of(here[axis], place)
        other = here[axis] + (1 - 2 * mine) * 2**place
        return (other, front) if axis == "leaf" else (leaf, other)

    all_bits = [("front", place) for place in range(front_bits)] + [("leaf", place) for place in range(3)]
    barrier = pltpu.get_barrier_semaphore()
    for bit in all_bits:
        pl.semaphore_signal(barrier, inc=1, device_id=partner(bit), device_id_type=MESH)
    loads = []
    for index in range(7):
        load = pltpu.make_async_copy(weights_hbm[index], weights[index], load_sems.at[index])
        load.start()
        loads.append(load)
    pl.semaphore_wait(barrier, len(all_bits))

    def unit(height):
        return LEAF_PIV // BLK if height == 0 else 1

    def slot_of(block, height, stripe):
        piece = unit(height)
        static = isinstance(block, int)
        place, rest = divmod(block, piece) if static else (block, 0)
        order = stripe_orders(front_bits, height)[stripe % 2]
        slot = 0
        for axis, at in order:
            at = at + height if axis == "front" else at
            slot = slot * 2 + (place >> at & 1 if static else bit_of(place, at))
        return slot * piece + rest

    def remote(source, target, bit):
        index = used[0]
        used[0] += 1
        copy = pltpu.make_async_remote_copy(
            src_ref=source,
            dst_ref=target,
            send_sem=send_sems.at[index],
            recv_sem=recv_sems.at[index],
            device_id=partner(bit),
            device_id_type=MESH,
        )
        copy.start()
        return copy

    def own_slots(height):
        out = []
        for stripe in range(stripes):
            slot = 0
            for axis, at in stripe_orders(front_bits, height)[stripe % 2]:
                slot = slot * 2 + bit_of(here[axis], at)
            out.append(slot * unit(height))
        return out

    def reduce_group(height, bufs, recvs, middle):
        piece = unit(height)
        orders = stripe_orders(front_bits, height)
        depth = len(orders[0])
        bases = [jnp.int32(0)] * stripes
        half = 2**depth * piece
        offset = 0
        for step in range(depth + 1):
            copies = []
            whole, half = half, half // 2
            for stripe in range(stripes):
                if step > 0:
                    pending[stripe].wait()
                    keep = bases[stripe]

                    def add(index, carry, stripe=stripe, keep=keep, prior=prior):
                        bufs[stripe][keep + index] += recvs[stripe][prior + index]
                        return carry

                    lax.fori_loop(0, whole, add, 0)
                if step < depth:
                    bit = orders[stripe % 2][step]
                    mine = bit_of(here[bit[0]], bit[1])
                    away = bases[stripe] + (1 - mine) * half
                    bases[stripe] = bases[stripe] + mine * half
                    copies.append(
                        remote(bufs[stripe].at[pl.ds(away, half)], recvs[stripe].at[pl.ds(offset, half)], bit)
                    )
            if step == 0:
                middle()
            pending, prior = copies, offset
            offset += half

    def gather_group(height, bufs, middle):
        piece = unit(height)
        orders = stripe_orders(front_bits, height)
        depth = len(orders[0])
        bases = own_slots(height)
        size = piece
        pending = None
        for step in range(depth, -1, -1):
            copies = []
            if step == 0:
                middle()
            for stripe in range(stripes):
                if pending is not None:
                    pending[stripe].wait()
                if step > 0:
                    bit = orders[stripe % 2][step - 1]
                    span = pl.ds(bases[stripe], size)
                    copies.append(remote(bufs[stripe].at[span], bufs[stripe].at[span], bit))
                    bases[stripe] = bases[stripe] - bit_of(here[bit[0]], bit[1]) * size
            pending = copies
            size *= 2

    def splits(height):
        return unit(height) == 1 and 2**height % CHUNK == 0

    def chunks(height, side, body, carry):
        count = sizes[height] // BLK // CHUNK
        if unit(height) > 1:
            for index in range(count):
                slots = [
                    [slot_of(index * CHUNK + step, height, kind) for kind in range(2)] for step in range(CHUNK)
                ]
                carry = body(index * CHUNK * BLK, slots, carry)
            return carry

        def visit(index, carry):
            if side is not None:
                run = 2**height // CHUNK
                index = lax.div(index, jnp.int32(run)) * (2 * run) + side * run + lax.rem(index, jnp.int32(run))
            bases = [slot_of(index * CHUNK, height, kind) for kind in range(2)]
            slots = [[bases[kind] + slot_of(step, height, kind) for kind in range(2)] for step in range(CHUNK)]
            return body(pl.multiple_of(index * (CHUNK * BLK), CHUNK * BLK), slots, carry)

        return lax.fori_loop(0, count if side is None else count // 2, visit, carry)

    def apply_rows(weight, bufs, height, side, total):
        def body(start, slots, total):
            parts = [
                jnp.concatenate([bufs[s][slots[step][s % 2]] for s in range(stripes)], axis=0)
                for step in range(CHUNK)
            ]
            left = split(jnp.concatenate(parts, axis=1))
            return total + product(left, weight[:, pl.ds(start, CHUNK * BLK)], 1)

        return chunks(height, side, body, total)

    def apply_cols(weight, vector, bufs, height, side):
        left = split(vector)

        def body(start, slots, carry):
            result = product(left, weight[:, pl.ds(start, CHUNK * BLK)], 0)
            for step in range(CHUNK):
                low = 0
                for s in range(stripes):
                    bufs[s][slots[step][s % 2]] = result[low : low + stripe_rows[s], step * BLK : (step + 1) * BLK]
                    low += stripe_rows[s]
            return carry

        chunks(height, side, body, 0)

    core = bit_of(front, 0)

    def reduced(weight, vector, height, recvs):
        if splits(height):
            apply_cols(weight, vector, partial, height, 1 - core)
            reduce_group(
                height, partial, recvs, lambda: apply_cols(weight, vector, partial, height, core)
            )
        else:
            apply_cols(weight, vector, partial, height, None)
            reduce_group(height, partial, recvs, lambda: None)

    def gathered_rows(weight, bufs, height, ready):
        totals = [jnp.zeros((BLK, weight.shape[0]), jnp.float32)]

        def own_side():
            ready()
            if splits(height):
                totals.append(apply_rows(weight, bufs, height, core, totals[-1]))

        gather_group(height, bufs, own_side)
        return apply_rows(weight, bufs, height, 1 - core if splits(height) else None, totals[-1])

    def own_block(bufs, slots, part):
        return jnp.concatenate([bufs[s][slots[s] + part] for s in range(stripes)], axis=0)

    def set_block(bufs, slots, part, value):
        low = 0
        for s in range(stripes):
            bufs[s][slots[s] + part] = value[low : low + stripe_rows[s]]
            low += stripe_rows[s]

    inverses = (weights[0], weights[2], weights[4], weights[6])
    couplings = (weights[1], weights[3], weights[5])
    starts = (0, LEAF_PIV, LEAF_PIV + SEP_PIV, LEAF_PIV + 2 * SEP_PIV)
    for height in range(4):
        slots = own_slots(height)
        if height > 0:
            loads[2 * height - 1].wait()
            reduced(couplings[height - 1], solved[height - 1][...], height, up_recv[height])
        for part in range(unit(height)):
            low = starts[height] + part * BLK
            value = rhs_ref[low : low + BLK, :].T
            if height > 0:
                value = value - own_block(partial, slots, part)
            set_block(up[height], slots, part, value)
        solved[height][...] = gathered_rows(inverses[height], up[height], height, loads[2 * height].wait)
    for height in (3, 2, 1, 0):
        target = solved[height][...]
        if height < 3:
            target = target - gathered_rows(couplings[height], down[height + 1], height + 1, lambda: None)
        reduced(inverses[height], target, height, down_recv[height])
        slots = own_slots(height)
        for part in range(unit(height)):
            low = starts[height] + part * BLK
            value = own_block(partial, slots, part)
            out_ref[low : low + BLK, :] = value.T
            if height > 0:
                set_block(down[height], slots, part, value)


def solve(ordered, weights):
    leaves = lax.axis_size("leaf")
    fronts = lax.axis_size("front")
    front_bits = fronts.bit_length() - 1
    rhs_count = ordered.shape[1]
    stripe_rows = (rhs_count // STRIPES,) * STRIPES
    sizes = tuple(w.shape[1] for w in (weights[0], weights[2], weights[4], weights[6]))
    scratch = [pltpu.VMEM(w.shape, jnp.float32) for w in weights]

    def stripe_buffers(blocks):
        return [pltpu.VMEM((blocks, rows, BLK), jnp.float32) for rows in stripe_rows]

    counts = [size // BLK for size in sizes]
    copies = 0
    for height in range(4):
        copies += (2 if height == 0 else 4) * (front_bits + height) * len(stripe_rows)
    for blocks in counts + counts[1:] + [max(counts)] + counts[1:] + counts:
        scratch += stripe_buffers(blocks)
    scratch += [pltpu.VMEM((rhs_count, rows), jnp.float32) for rows in (LEAF_PIV, SEP_PIV, SEP_PIV, SEP_PIV)]
    scratch += [
        pltpu.SemaphoreType.DMA((7,)),
        pltpu.SemaphoreType.DMA((copies,)),
        pltpu.SemaphoreType.DMA((copies,)),
    ]
    vmem = pl.BlockSpec(memory_space=pltpu.VMEM)
    return pl.pallas_call(
        functools.partial(solve_kernel, front_bits, stripe_rows, sizes),
        out_shape=jax.ShapeDtypeStruct(ordered.shape, jnp.float32),
        in_specs=[vmem] + [pl.BlockSpec(memory_space=pl.ANY)] * 7,
        out_specs=vmem,
        scratch_shapes=scratch,
        compiler_params=pltpu.CompilerParams(
            collective_id=0, has_side_effects=True, vmem_limit_bytes=66 * 1024 * 1000
        ),
    )(ordered, *weights)


def per_device(
    app_rhs,
    pivot_source,
    row_owner,
    leaf_inverse,
    leaf_coupling,
    sep1_inverse,
    sep1_coupling,
    sep2_inverse,
    sep2_coupling,
    sep3_inverse,
):
    row_count = app_rhs.shape[0]
    rhs_count = app_rhs.shape[1]
    peer_count = lax.axis_size("leaf") * lax.axis_size("front")
    mean_rows = row_count // (peer_count // 2)
    slot_cap = mean_rows + max(1, mean_rows // 4)
    destination = row_owner // row_count
    send_index = destination * slot_cap + ranked_slots(destination, peer_count)
    anchor = pivot_source // row_count
    same_source = (anchor[:, None] == anchor[None, :]) & (
        pivot_source[None, :] < pivot_source[:, None]
    )
    recv_index = anchor * slot_cap + jnp.sum(same_source.astype(jnp.int32), axis=1)
    outgoing = (
        jnp.zeros((peer_count * slot_cap, rhs_count), jnp.float32).at[send_index].set(app_rhs)
    )
    ordered = move_rows(outgoing, slot_cap)[recv_index]
    weights = [
        w[0, 0]
        for w in (
            leaf_inverse,
            leaf_coupling,
            sep1_inverse,
            sep1_coupling,
            sep2_inverse,
            sep2_coupling,
            sep3_inverse,
        )
    ]
    pivot_order = solve(ordered, weights)
    returning = (
        jnp.zeros((peer_count * slot_cap, rhs_count), jnp.float32).at[recv_index].set(pivot_order)
    )
    returned = move_rows(returning, slot_cap)
    return returned[send_index]


def solution(mesh):
    in_specs = (
        P(("leaf", "front"), None),
        P(("leaf", "front")),
        P(("leaf", "front")),
        P("leaf", "front", None, None),
        P("leaf", "front", None, None),
        P("leaf", "front", None, None),
        P("leaf", "front", None, None),
        P("leaf", "front", None, None),
        P("leaf", "front", None, None),
        P("leaf", "front", None, None),
    )
    out_specs = P(("leaf", "front"), None)
    return jax.shard_map(
        per_device, mesh=mesh, in_specs=in_specs, out_specs=out_specs, check_vma=False
    )
```
